256 devices in a mesh: ep: 8 (over x, core), fsdp: 32 (over z, y).
Axes of the slice: x: 4, y: 4, z: 8, core: 2. Of those that a mesh axis runs over, the one named last changes fastest.
Arguments:
- train_gate: float32 [128, 2048, 768], P('ep', 'fsdp'), may hold values from -0.25 to 0.25
- other_gate: bfloat16 [128, 2048, 768], P('ep', 'fsdp'), may hold values from -0.0625 to 0.0625
- train_up: float32 [128, 2048, 768], P('ep', 'fsdp'), may hold values from -0.25 to 0.25
- other_up: bfloat16 [128, 2048, 768], P('ep', 'fsdp'), may hold values from -0.0625 to 0.0625
- router_weight: float32 [2048, 128], P('fsdp', 'ep'), may hold values from -0.125 to 0.125
- router_gain: float32 [2048], P('fsdp'), may hold values from 0.25 to 1.75
Outputs:
- ready_gate: bfloat16 [128, 2048, 768], P('ep', None, 'fsdp')
- ready_up: bfloat16 [128, 2048, 768], P('ep', None, 'fsdp')
- scale_gate: float32 [128, 768], P('ep', 'fsdp')
- scale_up: float32 [128, 768], P('ep', 'fsdp')
- serve_router: bfloat16 [2048, 128], replicated
The draws below stay inside these ranges and needn't reach their ends.
All inputs are finite; a program needn't handle non-finite values. Where the reference program divides by a largest or mean magnitude, that divisor is 1e-20 or more.
Results may differ from the reference program's by a relative error of at most 0.001.
Values may be sent and summed in bfloat16 or wider, within the bound.
No kernel may reach another device: no remote copies, remote signals or barrier semaphores. Data moves between devices by JAX's collectives and lax.ppermute only.
A program may use at most 128 MiB of HBM per device.

```python
import jax
import jax.numpy as jnp

EXPERTS = 128
D_MODEL = 2048
D_EXPERT = 768


def spiked(values, stream_key, source, target, parts, factor):
    def block_of(axis_at):
        return (jnp.arange(values.shape[axis_at]) // (values.shape[axis_at] // parts)).reshape((-1,) + (1,) * (values.ndim - 1 - axis_at))

    first = jax.random.permutation(stream_key, parts)[block_of(target)]
    second = (block_of(target) + parts // 2) % parts
    return jnp.where((block_of(source) == first) | (block_of(source) == second), factor * values, values)


def level_of(own_key, shape, split, least, top_value):
    def one(position, parts):
        draws = jax.random.uniform(jax.random.fold_in(jax.random.fold_in(own_key, 6), position), (parts,), jnp.float32, least / len(split), top_value / len(split))
        return jnp.repeat(jnp.exp(draws), shape[position] // parts).reshape((-1,) + (1,) * (len(shape) - position - 1))

    gain = one(*split[0])
    for cut in split[1:]:
        gain = gain * one(*cut)
    return gain


def normal_values(key, extent, deviation, bound, cuts=(), held_as=jnp.bfloat16):
    level = level_of(key, extent, cuts, -0.22, 0.18) if cuts else 1.0
    values = jax.random.normal(key, extent, jnp.float32) * deviation * level
    return jnp.minimum(jnp.maximum(values, -bound), bound).astype(held_as)


def noise_with(stream_key, shape, spread, reach, cuts, heavy, held_as=jnp.bfloat16):
    entries = spread * jax.random.normal(stream_key, shape, jnp.float32)
    if cuts:
        entries = entries * level_of(stream_key, shape, cuts, -0.22, 0.18)
    return jnp.clip(spiked(entries, jax.random.fold_in(stream_key, 3), *heavy), -reach, reach).astype(held_as)


def setup_inputs(seed: int = 0) -> dict:
    key_of = jax.random.split(jax.random.key(seed), 7)
    return {
        "train_gate": noise_with(key_of[0], (EXPERTS, D_MODEL, D_EXPERT), D_MODEL ** -0.5, 0.25, ((0, 8), (1, 32)), (1, 2, 32, 2.75), jnp.float32),
        "other_gate": normal_values(key_of[1], (EXPERTS, D_MODEL, D_EXPERT), (D_MODEL * 4) ** -0.5, 0.0625, ((0, 8), (1, 32))),
        "train_up": noise_with(key_of[2], (EXPERTS, D_MODEL, D_EXPERT), D_MODEL ** -0.5, 0.25, ((0, 8), (1, 32)), (1, 2, 32, 2.75), jnp.float32),
        "other_up": normal_values(key_of[3], (EXPERTS, D_MODEL, D_EXPERT), (D_MODEL * 4) ** -0.5, 0.0625, ((0, 8), (1, 32))),
        "router_weight": normal_values(key_of[4], (D_MODEL, EXPERTS), D_MODEL ** -0.5, 0.125, ((0, 32), (1, 8)), jnp.float32),
        "router_gain": jnp.clip(1.0 + 0.15 * jax.random.normal(key_of[5], (D_MODEL,), jnp.float32), 0.25, 1.75),
    }


def reference(train_gate, other_gate, train_up, other_up, router_weight, router_gain):
    latest_gate = train_gate + other_gate.astype(jnp.float32)
    latest_up = train_up + other_up.astype(jnp.float32)
    scale_gate = jnp.sum(jnp.abs(latest_gate), axis=1) / D_MODEL
    ready_gate = (latest_gate / jnp.expand_dims(scale_gate, 1)).astype(jnp.bfloat16)
    scale_up = jnp.sum(jnp.abs(latest_up), axis=1) / D_MODEL
    ready_up = (latest_up / jnp.expand_dims(scale_up, 1)).astype(jnp.bfloat16)
    serve_router = (router_weight * router_gain[:, None]).astype(jnp.bfloat16)
    return ready_gate, ready_up, scale_gate, scale_up, serve_router
```

```python
import functools

import jax
import jax.numpy as jnp
from jax import lax
from jax.experimental import pallas as pl
from jax.experimental.pallas import tpu as pltpu
from jax.sharding import PartitionSpec as P

POWER = 15
SPREAD = 5.0
LEAST = 1e-30
PAIR = 2


def coded(latest):
    mean = jnp.sum(jnp.abs(latest), axis=0, keepdims=True) * (1.0 / (latest.shape[0] * SPREAD))
    norm = jnp.maximum(mean, LEAST).astype(jnp.bfloat16).astype(jnp.float32)
    v = latest * (1.0 / norm)
    v2 = v * v
    v4 = v2 * v2
    v8 = v4 * v4
    return (v8 * v4) * (v2 * v), norm


def encode_kernel(parts, tg, og, tu, ou, out, codes, norms, norm_rows, sems, norm_sem):
    step = pl.program_id(0)
    steps = pl.num_programs(0)
    width = tg.shape[2] // parts
    rows = PAIR * width
    slot = lax.rem(step, 2)

    def copy(s, at):
        return pltpu.make_async_copy(
            codes.at[at], out.at[:, pl.ds(pl.multiple_of(s * rows, 8), rows), :], sems.at[at]
        )

    @pl.when(step == 0)
    def _():
        norms[...] = jnp.zeros_like(norms)

    @pl.when(step >= 2)
    def _():
        copy(step - 2, slot).wait()

    for p in range(PAIR):
        cg, ng = coded(tg[p] + og[p].astype(jnp.float32))
        cu, nu = coded(tu[p] + ou[p].astype(jnp.float32))
        both = jnp.concatenate([cg, cu], axis=0)
        turned = both.T.astype(jnp.bfloat16).reshape(parts, width, both.shape[0])
        codes[slot, :, p * width : (p + 1) * width, :] = turned
        at = (step * PAIR + p) * 2
        norms[pl.ds(at, 1), :] = ng
        norms[pl.ds(at + 1, 1), :] = nu
    copy(step, slot).start()

    @pl.when(step == steps - 1)
    def _():
        turned = norms[...].T.reshape(parts, width // 8, 8, 128)
        packed = turned[:, 0]
        for k in range(1, width // 8):
            packed = packed + pltpu.roll(turned[:, k], 32 * k, 2)
        norm_rows[...] = packed.astype(jnp.bfloat16)
        last = pltpu.make_async_copy(
            norm_rows, out.at[:, pl.ds(steps * rows, 8), :], norm_sem
        )
        last.start()
        copy(step - 1, 1 - slot).wait()
        copy(step, slot).wait()
        last.wait()


def encode(parts, tg, og, tu, ou):
    experts, mine, columns = tg.shape
    width = columns // parts
    block = lambda: pl.BlockSpec((PAIR, mine, columns), lambda s: (s, 0, 0))
    return pl.pallas_call(
        functools.partial(encode_kernel, parts),
        grid=(experts // PAIR,),
        in_specs=[block() for _ in range(4)],
        out_specs=pl.BlockSpec(memory_space=pl.ANY),
        out_shape=jax.ShapeDtypeStruct((parts, experts * width + 8, 2 * mine), jnp.bfloat16),
        scratch_shapes=[
            pltpu.VMEM((2, parts, PAIR * width, 2 * mine), jnp.bfloat16),
            pltpu.VMEM((128, columns), jnp.float32),
            pltpu.VMEM((parts, 8, 2 * mine), jnp.bfloat16),
            pltpu.SemaphoreType.DMA((2,)),
            pltpu.SemaphoreType.DMA,
        ],
        name="encode",
    )(tg, og, tu, ou)


def decode_kernel(code, norm, ready_g, ready_u, scale_g, scale_u, sums):
    step = pl.program_id(0)
    parts = code.shape[0]
    width = code.shape[1] // PAIR
    tiles = width // 8
    total = parts * code.shape[2] // 2
    lane = lax.broadcasted_iota(jnp.int32, (8, 128), 1)
    left = lane < 64

    @pl.when(step == 0)
    def _():
        sums[...] = jnp.zeros_like(sums)

    source = lax.broadcasted_iota(jnp.int32, (128, PAIR * tiles * 128), 0)
    goal = lax.broadcasted_iota(jnp.int32, (128, PAIR * tiles * 128), 1)
    tile, at = goal // 128, goal % 128
    wanted = 32 * (tile % tiles) + 2 * (step * PAIR + tile // tiles) + at // 64
    pick = (source == wanted).astype(jnp.bfloat16)
    spread = jnp.dot(norm[...].reshape(parts * 8, 128), pick, preferred_element_type=jnp.float32)
    spread = spread.reshape(parts, 8, PAIR * tiles * 128)

    c = code[...].astype(jnp.float32)
    for p in range(PAIR):
        outs_g, outs_u = [], []
        for k in range(tiles):
            at = p * tiles + k
            tile = c[:, at * 8 : (at + 1) * 8, :]
            size = jnp.exp2(jnp.log2(jnp.abs(tile)) * (1.0 / POWER))
            size = size * spread[:, :, at * 128 : (at + 1) * 128]
            acc = jnp.sum(size, axis=0)
            sg = jnp.sum(jnp.where(left, acc, 0.0), axis=1, keepdims=True) * (1.0 / total)
            su = jnp.sum(jnp.where(left, 0.0, acc), axis=1, keepdims=True) * (1.0 / total)
            chosen = 2 * (step * PAIR + p)
            sums[k * 8 : (k + 1) * 8, :] += jnp.where(
                lane == chosen, sg, jnp.where(lane == chosen + 1, su, 0.0)
            )
            size = size * jnp.where(left, 1.0 / sg, 1.0 / su)[None]
            y = jnp.where(tile < 0, -size, size).reshape(parts // 2, 2, 8, 128)
            turned = pltpu.roll(y.reshape(parts, 8, 128), 64, 2).reshape(parts // 2, 2, 8, 128)
            outs_g.append(jnp.where(left, y[:, 0], turned[:, 1]))
            outs_u.append(jnp.where(left, turned[:, 0], y[:, 1]))
        g = jnp.concatenate(outs_g, axis=1).astype(jnp.bfloat16)
        u = jnp.concatenate(outs_u, axis=1).astype(jnp.bfloat16)
        for t in range(parts // 2):
            ready_g[p, :, t * 128 : (t + 1) * 128] = g[t]
            ready_u[p, :, t * 128 : (t + 1) * 128] = u[t]

    @pl.when(step == pl.num_programs(0) - 1)
    def _():
        turned = jnp.concatenate(
            [sums[...], jnp.zeros((128 - width, 128), jnp.float32)], axis=0
        ).T
        turned = turned[:32].reshape(16, 2, 128)
        scale_g[...] = turned[:, 0, :width]
        scale_u[...] = turned[:, 1, :width]


def decode(experts, arrived):
    parts, rows, lanes = arrived.shape
    width = (rows - 8) // experts
    total = parts * lanes // 2
    ready = jax.ShapeDtypeStruct((experts, width, total), jnp.bfloat16)
    scale = jax.ShapeDtypeStruct((experts, width), jnp.float32)
    out = lambda: pl.BlockSpec((PAIR, width, total), lambda s: (s, 0, 0))
    small = lambda: pl.BlockSpec((experts, width), lambda s: (0, 0))
    return pl.pallas_call(
        decode_kernel,
        grid=(experts // PAIR,),
        in_specs=[
            pl.BlockSpec((parts, PAIR * width, lanes), lambda s: (0, s, 0)),
            pl.BlockSpec((parts, 8, lanes), lambda s: (0, experts * width // 8, 0)),
        ],
        out_specs=[out(), out(), small(), small()],
        out_shape=[ready, ready, scale, scale],
        scratch_shapes=[pltpu.VMEM((width, 128), jnp.float32)],
        name="decode",
    )(arrived, arrived)


def swapped(block, axis, bit):
    n = lax.axis_size(axis)
    other = lax.ppermute(block, axis, [(i, i ^ bit) for i in range(n)])
    high = (lax.axis_index(axis) & bit) != 0
    return jnp.where(high, other, block), jnp.where(high, block, other)


def gathered(block, axis):
    shape = block.shape
    bit = lax.axis_size(axis) // 2
    held = 1
    while bit:
        low, high = swapped(block, axis, bit)
        low, high = (a.reshape(held, -1, *shape[1:]) for a in (low, high))
        block = jnp.stack([low, high], axis=1).reshape(-1, *shape[1:])
        held *= 2
        bit //= 2
    return block


def per_device(train_gate, other_gate, train_up, other_up, router_weight, router_gain):
    experts, mine, columns = train_gate.shape
    parts = lax.axis_size("fsdp")
    codes = encode(parts, train_gate, other_gate, train_up, other_up)
    arrived = lax.all_to_all(codes, "fsdp", split_axis=0, concat_axis=0, tiled=True)

    rows, wide = router_weight.shape
    part = (router_weight * router_gain[:, None]).astype(jnp.bfloat16).T
    part = part.reshape(1, 8, -1)
    part, _ = lax.optimization_barrier((part, codes))
    group = gathered(part, "fsdp").reshape(parts, wide, rows)
    group = group.transpose(1, 0, 2).reshape(wide, parts * rows)
    serve_router = gathered(group, "ep").T

    ready_gate, ready_up, scale_gate, scale_up = decode(experts, arrived)
    return (
        jnp.swapaxes(ready_gate, 1, 2),
        jnp.swapaxes(ready_up, 1, 2),
        scale_gate,
        scale_up,
        serve_router,
    )


def solution(mesh):
    in_specs = (
        P("ep", "fsdp", None),
        P("ep", "fsdp", None),
        P("ep", "fsdp", None),
        P("ep", "fsdp", None),
        P("fsdp", "ep"),
        P("fsdp"),
    )
    out_specs = (
        P("ep", None, "fsdp"),
        P("ep", None, "fsdp"),
        P("ep", "fsdp"),
        P("ep", "fsdp"),
        P(),
    )
    return jax.shard_map(
        per_device, mesh=mesh, in_specs=in_specs, out_specs=out_specs, check_vma=False
    )
```

```python
import functools

import jax
import jax.numpy as jnp
from jax import lax
from jax.experimental import pallas as pl
from jax.experimental.pallas import tpu as pltpu
from jax.sharding import PartitionSpec as P

POWER = 15
SPREAD = 5.0
LEAST = 1e-30
SMALLEST = 2.0**-126
PAIR = 2
LANES = 128
MIB = 2**20


def coded(latest):
    mean = jnp.sum(jnp.abs(latest), axis=0, keepdims=True) * (1.0 / (latest.shape[0] * SPREAD))
    norm = jnp.maximum(mean, LEAST).astype(jnp.bfloat16).astype(jnp.float32)
    v = latest * (1.0 / norm)
    v2 = v * v
    v4 = v2 * v2
    v8 = v4 * v4
    return (v8 * v4) * (v2 * v), norm


def coded_pair(parts, tg, og, tu, ou, p):
    cg, ng = coded(tg[p] + og[p].astype(jnp.float32))
    cu, nu = coded(tu[p] + ou[p].astype(jnp.float32))
    turned = jnp.concatenate([cg, cu], axis=0).T.reshape(parts, -1, LANES)
    return turned, ng, nu


def first_kernel(parts, tg, og, tu, ou, weight, gain, out, norms):
    width = tg.shape[2] // parts
    rows = PAIR * width
    norms[...] = jnp.zeros_like(norms)
    for p in range(PAIR):
        codes, ng, nu = coded_pair(parts, tg, og, tu, ou, p)
        for k in range(0, width, 8):
            out[:, p * width + k : p * width + k + 8, :] = codes[:, k : k + 8].astype(jnp.bfloat16)
        norms[2 * p : 2 * p + 1, :] = ng
        norms[2 * p + 1 : 2 * p + 2, :] = nu
    part = weight[...] * gain[...]
    part = jnp.concatenate([part[:8], part[8:]], axis=1).astype(jnp.bfloat16)
    out[:, rows:, :] = jnp.broadcast_to(part[None], (parts, 8, LANES))


def encode_first(parts, tg, og, tu, ou, weight, gain):
    _, mine, columns = tg.shape
    width = columns // parts
    block = lambda: pl.BlockSpec((PAIR, mine, columns), lambda s: (0, 0, 0))
    whole = lambda a: pl.BlockSpec(a.shape, lambda s: (0,) * len(a.shape))
    out = jax.ShapeDtypeStruct((parts, PAIR * width + 8, LANES), jnp.bfloat16)
    norms = jax.ShapeDtypeStruct((8, columns), jnp.float32)
    return pl.pallas_call(
        functools.partial(first_kernel, parts),
        grid=(1,),
        in_specs=[block() for _ in range(4)] + [whole(weight), whole(gain)],
        out_specs=[whole(out), whole(norms)],
        out_shape=[out, norms],
        cost_estimate=pl.CostEstimate(flops=50_000_000, bytes_accessed=1_700_000, transcendentals=0),
        name="encode_first",
    )(tg, og, tu, ou, weight, gain)


def rest_kernel(parts, tg, og, tu, ou, before, out, codes, norms, norm_rows, sems, norm_sem):
    step = pl.program_id(0)
    steps = pl.num_programs(0)
    width = tg.shape[2] // parts
    rows = PAIR * width
    slot = lax.rem(step, 2)

    def copy(s, at):
        return pltpu.make_async_copy(
            codes.at[at], out.at[:, pl.ds(pl.multiple_of(s * rows, 8), rows), :], sems.at[at]
        )

    @pl.when(step == 0)
    def _():
        norms[...] = jnp.zeros_like(norms)
        norms[0:8, :] = before[...]

    @pl.when(step >= 2)
    def _():
        copy(step - 2, slot).wait()

    for p in range(PAIR):
        turned, ng, nu = coded_pair(parts, tg, og, tu, ou, p)
        for k in range(0, width, 8):
            codes[slot, :, p * width + k : p * width + k + 8, :] = turned[:, k : k + 8].astype(
                jnp.bfloat16
            )
        at = ((step + 1) * PAIR + p) * 2
        norms[pl.ds(at, 1), :] = ng
        norms[pl.ds(at + 1, 1), :] = nu
    copy(step, slot).start()

    @pl.when(step == steps - 1)
    def _():
        turned = norms[...].T.reshape(parts, width // 8, 8, LANES)
        packed = turned[:, 0]
        for k in range(1, width // 8):
            packed = packed + pltpu.roll(turned[:, k], 32 * k, 2)
        norm_rows[...] = packed.astype(jnp.bfloat16)
        last = pltpu.make_async_copy(
            norm_rows, out.at[:, pl.ds(steps * rows, 8), :], norm_sem
        )
        last.start()
        copy(step - 1, 1 - slot).wait()
        copy(step, slot).wait()
        last.wait()


def encode_rest(parts, tg, og, tu, ou, before):
    experts, mine, columns = tg.shape
    width = columns // parts
    steps = experts // PAIR - 1
    block = lambda: pl.BlockSpec((PAIR, mine, columns), lambda s: (s + 1, 0, 0))
    return pl.pallas_call(
        functools.partial(rest_kernel, parts),
        grid=(steps,),
        in_specs=[block() for _ in range(4)] + [pl.BlockSpec(before.shape, lambda s: (0, 0))],
        out_specs=pl.BlockSpec(memory_space=pl.ANY),
        out_shape=jax.ShapeDtypeStruct((parts, steps * PAIR * width + 8, LANES), jnp.bfloat16),
        scratch_shapes=[
            pltpu.VMEM((2, parts, PAIR * width, LANES), jnp.bfloat16),
            pltpu.VMEM((LANES, columns), jnp.float32),
            pltpu.VMEM((parts, 8, LANES), jnp.bfloat16),
            pltpu.SemaphoreType.DMA((2,)),
            pltpu.SemaphoreType.DMA,
        ],
        cost_estimate=pl.CostEstimate(flops=400_000_000, bytes_accessed=11_000_000, transcendentals=0),
        name="encode_rest",
    )(tg, og, tu, ou, before)


def decode_kernel(first, rest, out_g, out_u, scale_g, scale_u, pick, spread, values, sums, ready, sems):
    parts = first.shape[0]
    rows = first.shape[1] - 8
    width = rows // PAIR
    tiles = width // 8
    steps = rest.shape[1] // rows + 1
    total = parts * LANES // 2
    half = LANES // 2
    lane = lax.broadcasted_iota(jnp.int32, (rows, LANES), 1)
    left = lane < half
    sums[...] = jnp.zeros_like(sums)

    source = lax.broadcasted_iota(jnp.int32, pick.shape, 0)
    goal = lax.broadcasted_iota(jnp.int32, pick.shape, 1)
    tile, at = goal // LANES, goal % LANES
    wanted = 32 * (tile % tiles) + 2 * (tile // tiles) + at // half
    pick[...] = (source == wanted).astype(jnp.bfloat16)

    def copies(step, slot):
        where = pl.ds(pl.multiple_of(step * rows, rows), rows)
        return [
            pltpu.make_async_copy(ready.at[slot, m], out.at[where, :], sems.at[slot, m])
            for m, out in enumerate((out_g, out_u))
        ]

    def one(step, code, start):
        slot = lax.rem(step, 2)
        norm = rest[:, (steps - 1) * rows :, :].reshape(parts * 8, LANES).astype(jnp.float32)
        norm = pltpu.roll(norm, lax.rem(LANES - 2 * PAIR * step, LANES), 1)
        spread[...] = jnp.dot(
            norm.astype(jnp.bfloat16), pick[...], preferred_element_type=jnp.float32
        )
        acc = jnp.zeros((rows, LANES), jnp.float32)
        for src in range(parts):
            c = code[src, pl.ds(start, rows), :].astype(jnp.float32)
            scale = jnp.concatenate(
                [
                    spread[src * 8 : src * 8 + 8, k * LANES : (k + 1) * LANES]
                    for k in range(PAIR * tiles)
                ],
                axis=0,
            )
            size = jnp.log2(jnp.maximum(jnp.abs(c), SMALLEST))
            value = (c * scale) * jnp.exp2(size * (1.0 / POWER - 1.0))
            acc = acc + jnp.abs(value)
            values[src] = value
        sg = jnp.sum(jnp.where(left, acc, 0.0), axis=1, keepdims=True) * (1.0 / total)
        su = jnp.sum(jnp.where(left, 0.0, acc), axis=1, keepdims=True) * (1.0 / total)
        sums[...] += jnp.where(
            lane == 2 * step, sg, jnp.where(lane == 2 * step + 1, su, 0.0)
        )
        factor = jnp.where(left, 1.0 / sg, 1.0 / su)

        @pl.when(step >= 2)
        def _():
            for copy in copies(step - 2, slot):
                copy.wait()

        for t in range(parts // 2):
            even, odd = values[2 * t] * factor, values[2 * t + 1] * factor
            g = jnp.where(left, even, pltpu.roll(odd, half, 1))
            u = jnp.where(left, pltpu.roll(even, half, 1), odd)
            for m, whole in enumerate((g, u)):
                for k in range(0, rows, 8):
                    ready[slot, m, k : k + 8, t * LANES : (t + 1) * LANES] = whole[
                        k : k + 8
                    ].astype(jnp.bfloat16)
        for copy in copies(step, slot):
            copy.start()

    one(jnp.int32(0), first, 0)

    @pl.loop(1, steps)
    def _(step):
        one(step, rest, pl.multiple_of((step - 1) * rows, 8))

    turned = jnp.concatenate(
        [sums[...], jnp.zeros((LANES - rows, LANES), jnp.float32)], axis=0
    ).T
    turned = turned[: 2 * steps].reshape(steps, 2, LANES)
    for p in range(PAIR):
        scale_g[pl.ds(p, steps, stride=PAIR), :] = turned[:, 0, p * width : (p + 1) * width]
        scale_u[pl.ds(p, steps, stride=PAIR), :] = turned[:, 1, p * width : (p + 1) * width]
    for step in (steps - 2, steps - 1):
        for copy in copies(step, step % 2):
            copy.wait()


def decode(experts, first, rest):
    parts, rows, lanes = first.shape
    rows = rows - 8
    width = rows // PAIR
    total = parts * lanes // 2
    ready = jax.ShapeDtypeStruct((experts * width, total), jnp.bfloat16)
    scale = jax.ShapeDtypeStruct((experts, width), jnp.float32)
    vmem, anywhere = pl.BlockSpec(memory_space=pltpu.VMEM), pl.BlockSpec(memory_space=pl.ANY)
    ready_g, ready_u, scale_g, scale_u = pl.pallas_call(
        decode_kernel,
        in_specs=[vmem, vmem],
        out_specs=[anywhere, anywhere, vmem, vmem],
        out_shape=[ready, ready, scale, scale],
        scratch_shapes=[
            pltpu.VMEM((lanes, rows // 8 * lanes), jnp.bfloat16),
            pltpu.VMEM((parts * 8, rows // 8 * lanes), jnp.float32),
            pltpu.VMEM((parts, rows, lanes), jnp.float32),
            pltpu.VMEM((rows, lanes), jnp.float32),
            pltpu.VMEM((2, 2, rows, total), jnp.bfloat16),
            pltpu.SemaphoreType.DMA((2, 2)),
        ],
        compiler_params=pltpu.CompilerParams(vmem_limit_bytes=20 * MIB),
        cost_estimate=pl.CostEstimate(
            flops=400_000_000, bytes_accessed=6_400_000, transcendentals=3_200_000
        ),
        name="decode",
    )(first, rest)
    back = lambda a: jnp.swapaxes(a.reshape(experts, width, total), 1, 2)
    return back(ready_g), back(ready_u), scale_g, scale_u


def gathered(block, axis):
    n, held = lax.axis_size(axis), block[None]
    bit = n // 2
    while bit:
        other = lax.ppermute(held, axis, [(i, i ^ bit) for i in range(n)])
        high = (lax.axis_index(axis) & bit) != 0
        low, top = jnp.where(high, other, held), jnp.where(high, held, other)
        held = jnp.stack([low, top], axis=1).reshape(-1, *block.shape)
        bit //= 2
    return held


def per_device(train_gate, other_gate, train_up, other_up, router_weight, router_gain):
    experts = train_gate.shape[0]
    parts = lax.axis_size("fsdp")
    latest = (train_gate, other_gate, train_up, other_up)
    sent = lambda a: lax.all_to_all(a, "fsdp", split_axis=0, concat_axis=0, tiled=True)

    codes, norms = encode_first(parts, *latest, router_weight.T, router_gain[None])
    first = sent(codes)
    rest = sent(encode_rest(parts, *latest, norms))

    router = gathered(first[:, -8:, :], "ep")
    groups, half = router.shape[0], LANES // 2
    router = router.reshape(groups, parts, 8, 2, half).transpose(1, 4, 0, 3, 2)
    serve_router = router.reshape(parts * half, groups * 16)

    return (*decode(experts, first, rest), serve_router)


def solution(mesh):
    in_specs = (
        P("ep", "fsdp", None),
        P("ep", "fsdp", None),
        P("ep", "fsdp", None),
        P("ep", "fsdp", None),
        P("fsdp", "ep"),
        P("fsdp"),
    )
    out_specs = (
        P("ep", None, "fsdp"),
        P("ep", None, "fsdp"),
        P("ep", "fsdp"),
        P("ep", "fsdp"),
        P(),
    )
    return jax.shard_map(
        per_device, mesh=mesh, in_specs=in_specs, out_specs=out_specs, check_vma=False
    )
```

```python
import functools

import jax
import jax.numpy as jnp
from jax import lax
from jax.experimental import pallas as pl
from jax.experimental.pallas import tpu as pltpu
from jax.sharding import PartitionSpec as P

POWER = 15
SPREAD = 5.0
LEAST = 1e-30
SMALLEST = 2.0**-126
PAIR = 2
LANES = 128
MIB = 2**20


def coded(latest):
    mean = jnp.sum(jnp.abs(latest), axis=0, keepdims=True) * (1.0 / (latest.shape[0] * SPREAD))
    norm = jnp.maximum(mean, LEAST).astype(jnp.bfloat16).astype(jnp.float32)
    v = latest * (1.0 / norm)
    v2 = v * v
    v4 = v2 * v2
    v8 = v4 * v4
    return (v8 * v4) * (v2 * v), norm


def coded_expert(parts, tg, og, tu, ou):
    cg, ng = coded(tg[...] + og[...].astype(jnp.float32))
    cu, nu = coded(tu[...] + ou[...].astype(jnp.float32))
    return jnp.concatenate([cg, cu], axis=0).T.reshape(parts, -1, LANES), ng, nu


def first_kernel(parts, tg, og, tu, ou, weight, gain, out, norms):
    width = tg.shape[2] // parts
    norms[...] = jnp.zeros_like(norms)
    part = weight[...] * gain[...]
    part = jnp.concatenate([part[:8], part[8:]], axis=1).astype(jnp.bfloat16)
    out[:, width:, :] = jnp.broadcast_to(part[None], (parts, 8, LANES))
    codes, norms[0:1, :], norms[1:2, :] = coded_expert(
        parts, *(a.at[0] for a in (tg, og, tu, ou))
    )
    for k in range(0, width, 8):
        out[:, k : k + 8, :] = codes[:, k : k + 8].astype(jnp.bfloat16)


def encode_first(parts, tg, og, tu, ou, weight, gain):
    _, mine, columns = tg.shape
    width = columns // parts
    block = lambda: pl.BlockSpec((1, mine, columns), lambda s: (0, 0, 0))
    whole = lambda a: pl.BlockSpec(a.shape, lambda s: (0,) * len(a.shape))
    out = jax.ShapeDtypeStruct((parts, width + 8, LANES), jnp.bfloat16)
    norms = jax.ShapeDtypeStruct((8, columns), jnp.float32)
    return pl.pallas_call(
        functools.partial(first_kernel, parts),
        grid=(1,),
        in_specs=[block() for _ in range(4)] + [whole(weight), whole(gain)],
        out_specs=[whole(out), whole(norms)],
        out_shape=[out, norms],
        cost_estimate=pl.CostEstimate(flops=25_000_000, bytes_accessed=900_000, transcendentals=0),
        name="encode_first",
    )(tg, og, tu, ou, weight, gain)


def rest_kernel(parts, tg, og, tu, ou, before, out, ins, codes, norms, norm_rows, in_sems, sems, norm_sem):
    count = codes.shape[0]
    width = codes.shape[2]

    def reads(e):
        return [
            pltpu.make_async_copy(a.at[e + 1], held.at[e], in_sems.at[e, m])
            for m, (a, held) in enumerate(zip((tg, og, tu, ou), ins))
        ]

    def copy(e):
        return pltpu.make_async_copy(
            codes.at[e], out.at[:, pl.ds(pl.multiple_of(e * width, 8), width), :], sems.at[e]
        )

    @pl.loop(0, count)
    def _(e):
        for read in reads(e):
            read.start()

    norms[...] = jnp.zeros_like(norms)
    norms[0:8, :] = before[...]

    @pl.loop(0, count)
    def _(e):
        for read in reads(e):
            read.wait()
        turned, ng, nu = coded_expert(parts, *(held.at[e] for held in ins))
        for k in range(0, width, 8):
            codes[e, :, k : k + 8, :] = turned[:, k : k + 8].astype(jnp.bfloat16)
        norms[pl.ds(2 * e + 2, 1), :] = ng
        norms[pl.ds(2 * e + 3, 1), :] = nu
        copy(e).start()

    turned = norms[...].T.reshape(parts, width // 8, 8, LANES)
    packed = turned[:, 0]
    for k in range(1, width // 8):
        packed = packed + pltpu.roll(turned[:, k], 32 * k, 2)
    norm_rows[...] = packed.astype(jnp.bfloat16)
    last = pltpu.make_async_copy(norm_rows, out.at[:, pl.ds(count * width, 8), :], norm_sem)
    last.start()

    @pl.loop(0, count)
    def _(e):
        copy(e).wait()

    last.wait()


def encode_rest(parts, tg, og, tu, ou, before):
    experts, mine, columns = tg.shape
    width = columns // parts
    count = experts - 1
    vmem, anywhere = pl.BlockSpec(memory_space=pltpu.VMEM), pl.BlockSpec(memory_space=pl.ANY)

    def kernel(tg, og, tu, ou, before, out, a, b, c, d, *scratch):
        rest_kernel(parts, tg, og, tu, ou, before, out, (a, b, c, d), *scratch)

    return pl.pallas_call(
        kernel,
        in_specs=[anywhere] * 4 + [vmem],
        out_specs=anywhere,
        out_shape=jax.ShapeDtypeStruct((parts, count * width + 8, LANES), jnp.bfloat16),
        scratch_shapes=[
            *[pltpu.VMEM((count, mine, columns), a.dtype) for a in (tg, og, tu, ou)],
            pltpu.VMEM((count, parts, width, LANES), jnp.bfloat16),
            pltpu.VMEM((LANES, columns), jnp.float32),
            pltpu.VMEM((parts, 8, LANES), jnp.bfloat16),
            pltpu.SemaphoreType.DMA((count, 4)),
            pltpu.SemaphoreType.DMA((count,)),
            pltpu.SemaphoreType.DMA,
        ],
        cost_estimate=pl.CostEstimate(flops=400_000_000, bytes_accessed=11_000_000, transcendentals=0),
        name="encode_rest",
    )(tg, og, tu, ou, before)


def decode_kernel(
    first, rest, out_g, out_u, scale_g, scale_u, pick, sums, ready, sems, scales, scale_sems, *pairs
):
    spreads, values, factors = pairs[0:2], pairs[2:4], pairs[4:6]
    parts = first.shape[0]
    width = first.shape[1] - 8
    rows = width * PAIR
    tiles = width // 8
    steps = (rest.shape[1] - 8 + width) // rows
    total = parts * LANES // 2
    half = LANES // 2
    lane = lax.broadcasted_iota(jnp.int32, (8, LANES), 1)
    left = lane < half
    sums[...] = jnp.zeros_like(sums)

    source = lax.broadcasted_iota(jnp.int32, pick.shape, 0)
    goal = lax.broadcasted_iota(jnp.int32, pick.shape, 1)
    tile, at = goal // LANES, goal % LANES
    wanted = 32 * (tile % tiles) + 2 * (tile // tiles) + at // half
    pick[...] = (source == wanted).astype(jnp.bfloat16)

    def copies(step, slot):
        where = pl.ds(pl.multiple_of(step * rows, rows), rows)
        return [
            pltpu.make_async_copy(ready.at[slot, m], out.at[where, :], sems.at[slot, m])
            for m, out in enumerate((out_g, out_u))
        ]

    def spread_norms(step, side):
        norm = rest[:, steps * rows - width :, :].reshape(parts * 8, LANES).astype(jnp.float32)
        norm = pltpu.roll(norm, lax.rem(LANES - 2 * PAIR * step, LANES), 1)
        spreads[side][...] = jnp.dot(
            norm.astype(jnp.bfloat16), pick[...], preferred_element_type=jnp.float32
        )

    def read(step, side, codes_of):
        acc = [jnp.zeros((8, LANES), jnp.float32) for _ in range(PAIR * tiles)]
        for src in range(parts):
            whole = codes_of(src).astype(jnp.float32)
            for k in range(PAIR * tiles):
                c = whole[8 * k : 8 * k + 8]
                scale = spreads[side][src * 8 : src * 8 + 8, k * LANES : (k + 1) * LANES]
                size = jnp.log2(jnp.maximum(jnp.abs(c), SMALLEST))
                value = (c * scale) * jnp.exp2(size * (1.0 / POWER - 1.0))
                acc[k] = acc[k] + jnp.abs(value)
                values[side][src, 8 * k : 8 * k + 8, :] = value
        for k in range(PAIR * tiles):
            at = slice(8 * k, 8 * k + 8)
            sg = jnp.sum(jnp.where(left, acc[k], 0.0), axis=1, keepdims=True) * (1.0 / total)
            su = jnp.sum(jnp.where(left, 0.0, acc[k]), axis=1, keepdims=True) * (1.0 / total)
            sums[at, :] += jnp.where(
                lane == 2 * step, sg, jnp.where(lane == 2 * step + 1, su, 0.0)
            )
            factors[side][at, :] = 1.0 / jnp.where(left, sg, su)

    def write(step, side):
        for t in range(parts // 2):
            for k in range(PAIR * tiles):
                at = slice(8 * k, 8 * k + 8)
                factor = factors[side][at, :]
                even = values[side][2 * t, at, :] * factor
                odd = values[side][2 * t + 1, at, :] * factor
                g = jnp.where(left, even, pltpu.roll(odd, half, 1))
                u = jnp.where(left, pltpu.roll(even, half, 1), odd)
                for m, whole in enumerate((g, u)):
                    ready[side, m, at, t * LANES : (t + 1) * LANES] = whole.astype(jnp.bfloat16)
        for copy in copies(step, side):
            copy.start()

    def wait(step, side):
        for copy in copies(step, side):
            copy.wait()

    def from_rest(step, side):
        start = pl.multiple_of(step * rows - width, 8)
        read(step, side, lambda src: rest[src, pl.ds(start, rows), :])

    spread_norms(jnp.int32(0), 0)
    spread_norms(jnp.int32(1), 1)
    read(
        jnp.int32(0),
        0,
        lambda src: jnp.concatenate([first[src, :width, :], rest[src, :width, :]], axis=0),
    )

    @pl.loop(0, steps // 2 - 1)
    def _(i):
        for side in (1, 0):
            step = 2 * i + 2 - side

            @pl.when(i > 0)
            def _():
                wait(step - 3, 1 - side)

            write(step - 1, 1 - side)
            spread_norms(step + 1, 1 - side)
            from_rest(step, side)

    last = steps - 1
    wait(last - 3, 0)
    write(last - 1, 0)
    from_rest(jnp.int32(last), 1)
    turned = jnp.concatenate(
        [sums[...], jnp.zeros((LANES - rows, LANES), jnp.float32)], axis=0
    ).T
    turned = turned[: 2 * steps].reshape(steps, 2, LANES)
    scale_copies = []
    for m, out in enumerate((scale_g, scale_u)):
        for p in range(PAIR):
            scales[m, pl.ds(p, steps, stride=PAIR), :] = turned[:, m, p * width : (p + 1) * width]
        scale_copies.append(pltpu.make_async_copy(scales.at[m], out, scale_sems.at[m]))
        scale_copies[m].start()
    wait(last - 2, 1)
    write(last, 1)
    wait(last - 1, 0)
    wait(last, 1)
    for copy in scale_copies:
        copy.wait()


def decode(experts, first, rest):
    parts, rows, lanes = first.shape
    width = rows - 8
    rows = width * PAIR
    total = parts * lanes // 2
    ready = jax.ShapeDtypeStruct((experts * width, total), jnp.bfloat16)
    scale = jax.ShapeDtypeStruct((experts, width), jnp.float32)
    vmem, anywhere = pl.BlockSpec(memory_space=pltpu.VMEM), pl.BlockSpec(memory_space=pl.ANY)
    ready_g, ready_u, scale_g, scale_u = pl.pallas_call(
        decode_kernel,
        in_specs=[vmem, vmem],
        out_specs=[anywhere] * 4,
        out_shape=[ready, ready, scale, scale],
        scratch_shapes=[
            pltpu.VMEM((lanes, rows // 8 * lanes), jnp.bfloat16),
            pltpu.VMEM((rows, lanes), jnp.float32),
            pltpu.VMEM((2, 2, rows, total), jnp.bfloat16),
            pltpu.SemaphoreType.DMA((2, 2)),
            pltpu.VMEM((2, experts, width), jnp.float32),
            pltpu.SemaphoreType.DMA((2,)),
            *[pltpu.VMEM((parts * 8, rows // 8 * lanes), jnp.float32)] * 2,
            *[pltpu.VMEM((parts, rows, lanes), jnp.float32)] * 2,
            *[pltpu.VMEM((rows, lanes), jnp.float32)] * 2,
        ],
        compiler_params=pltpu.CompilerParams(vmem_limit_bytes=20 * MIB),
        cost_estimate=pl.CostEstimate(
            flops=400_000_000, bytes_accessed=6_400_000, transcendentals=3_200_000
        ),
        name="decode",
    )(first, rest)
    back = lambda a: jnp.swapaxes(a.reshape(experts, width, total), 1, 2)
    return back(ready_g), back(ready_u), scale_g, scale_u


def gathered(block, axis):
    n, held = lax.axis_size(axis), block[None]
    bit = n // 2
    while bit:
        other = lax.ppermute(held, axis, [(i, i ^ bit) for i in range(n)])
        high = (lax.axis_index(axis) & bit) != 0
        low, top = jnp.where(high, other, held), jnp.where(high, held, other)
        held = jnp.stack([low, top], axis=1).reshape(-1, *block.shape)
        bit //= 2
    return held


def per_device(train_gate, other_gate, train_up, other_up, router_weight, router_gain):
    experts = train_gate.shape[0]
    parts = lax.axis_size("fsdp")
    latest = (train_gate, other_gate, train_up, other_up)
    sent = lambda a: lax.all_to_all(a, "fsdp", split_axis=0, concat_axis=0, tiled=True)

    codes, norms = encode_first(parts, *latest, router_weight.T, router_gain[None])
    first = sent(codes)
    rest = sent(encode_rest(parts, *latest, norms))

    router = gathered(first[:, -8:, :], "ep")
    groups, half = router.shape[0], LANES // 2
    router = router.reshape(groups, parts, 8, 2, half).transpose(1, 4, 0, 3, 2)
    serve_router = router.reshape(parts * half, groups * 16)

    return (*decode(experts, first, rest), serve_router)


def solution(mesh):
    in_specs = (
        P("ep", "fsdp", None),
        P("ep", "fsdp", None),
        P("ep", "fsdp", None),
        P("ep", "fsdp", None),
        P("fsdp", "ep"),
        P("fsdp"),
    )
    out_specs = (
        P("ep", None, "fsdp"),
        P("ep", None, "fsdp"),
        P("ep", "fsdp"),
        P("ep", "fsdp"),
        P(),
    )
    return jax.shard_map(
        per_device, mesh=mesh, in_specs=in_specs, out_specs=out_specs, check_vma=False
    )
```

```python
import functools

import jax
import jax.numpy as jnp
from jax import lax
from jax.experimental import pallas as pl
from jax.experimental.pallas import tpu as pltpu
from jax.sharding import PartitionSpec as P

POWER = 15
SPREAD = 5.0
LEAST = 1e-30
SMALLEST = 2.0**-126
PAIR = 2
LANES = 128
MIB = 2**20


def coded(latest):
    mean = jnp.sum(jnp.abs(latest), axis=0, keepdims=True) * (1.0 / (latest.shape[0] * SPREAD))
    norm = jnp.maximum(mean, LEAST).astype(jnp.bfloat16).astype(jnp.float32)
    v = latest * (1.0 / norm)
    v2 = v * v
    v4 = v2 * v2
    v8 = v4 * v4
    return (v8 * v4) * (v2 * v), norm


def coded_expert(parts, tg, og, tu, ou):
    cg, ng = coded(tg[...] + og[...].astype(jnp.float32))
    cu, nu = coded(tu[...] + ou[...].astype(jnp.float32))
    return jnp.concatenate([cg, cu], axis=0).T.reshape(parts, -1, LANES), ng, nu


def first_kernel(parts, tg, og, tu, ou, weight, gain, out, norms):
    width = tg.shape[2] // parts
    norms[...] = jnp.zeros_like(norms)
    part = weight[...] * gain[...]
    part = jnp.concatenate([part[:8], part[8:]], axis=1).astype(jnp.bfloat16)
    out[:, width:, :] = jnp.broadcast_to(part[None], (parts, 8, LANES))
    codes, norms[0:1, :], norms[1:2, :] = coded_expert(
        parts, *(a.at[0] for a in (tg, og, tu, ou))
    )
    for k in range(0, width, 8):
        out[:, k : k + 8, :] = codes[:, k : k + 8].astype(jnp.bfloat16)


def encode_first(parts, tg, og, tu, ou, weight, gain):
    _, mine, columns = tg.shape
    width = columns // parts
    block = lambda: pl.BlockSpec((1, mine, columns), lambda s: (0, 0, 0))
    whole = lambda a: pl.BlockSpec(a.shape, lambda s: (0,) * len(a.shape))
    out = jax.ShapeDtypeStruct((parts, width + 8, LANES), jnp.bfloat16)
    norms = jax.ShapeDtypeStruct((8, columns), jnp.float32)
    return pl.pallas_call(
        functools.partial(first_kernel, parts),
        grid=(1,),
        in_specs=[block() for _ in range(4)] + [whole(weight), whole(gain)],
        out_specs=[whole(out), whole(norms)],
        out_shape=[out, norms],
        cost_estimate=pl.CostEstimate(flops=25_000_000, bytes_accessed=900_000, transcendentals=0),
        name="encode_first",
    )(tg, og, tu, ou, weight, gain)


def rest_kernel(parts, tg, og, tu, ou, before, out, ins, codes, norms, norm_rows, in_sems, sems, norm_sem):
    count = codes.shape[0]
    width = codes.shape[2]

    def reads(e):
        return [
            pltpu.make_async_copy(a.at[e + 1], held.at[e], in_sems.at[e, m])
            for m, (a, held) in enumerate(zip((tg, og, tu, ou), ins))
        ]

    def copy(e):
        return pltpu.make_async_copy(
            codes.at[e], out.at[:, pl.ds(pl.multiple_of(e * width, 8), width), :], sems.at[e]
        )

    @pl.loop(0, count)
    def _(e):
        for read in reads(e):
            read.start()

    norms[...] = jnp.zeros_like(norms)
    norms[0:8, :] = before[...]

    @pl.loop(0, count)
    def _(e):
        for read in reads(e):
            read.wait()
        turned, ng, nu = coded_expert(parts, *(held.at[e] for held in ins))
        for k in range(0, width, 8):
            codes[e, :, k : k + 8, :] = turned[:, k : k + 8].astype(jnp.bfloat16)
        norms[pl.ds(2 * e + 2, 1), :] = ng
        norms[pl.ds(2 * e + 3, 1), :] = nu
        copy(e).start()

    turned = norms[...].T.reshape(parts, width // 8, 8, LANES)
    packed = turned[:, 0]
    for k in range(1, width // 8):
        packed = packed + pltpu.roll(turned[:, k], 32 * k, 2)
    norm_rows[...] = packed.astype(jnp.bfloat16)
    last = pltpu.make_async_copy(norm_rows, out.at[:, pl.ds(count * width, 8), :], norm_sem)
    last.start()

    @pl.loop(0, count)
    def _(e):
        copy(e).wait()

    last.wait()


def encode_rest(parts, tg, og, tu, ou, before):
    experts, mine, columns = tg.shape
    width = columns // parts
    count = experts - 1
    vmem, anywhere = pl.BlockSpec(memory_space=pltpu.VMEM), pl.BlockSpec(memory_space=pl.ANY)

    def kernel(tg, og, tu, ou, before, out, a, b, c, d, *scratch):
        rest_kernel(parts, tg, og, tu, ou, before, out, (a, b, c, d), *scratch)

    return pl.pallas_call(
        kernel,
        in_specs=[anywhere] * 4 + [vmem],
        out_specs=anywhere,
        out_shape=jax.ShapeDtypeStruct((parts, count * width + 8, LANES), jnp.bfloat16),
        scratch_shapes=[
            *[pltpu.VMEM((count, mine, columns), a.dtype) for a in (tg, og, tu, ou)],
            pltpu.VMEM((count, parts, width, LANES), jnp.bfloat16),
            pltpu.VMEM((LANES, columns), jnp.float32),
            pltpu.VMEM((parts, 8, LANES), jnp.bfloat16),
            pltpu.SemaphoreType.DMA((count, 4)),
            pltpu.SemaphoreType.DMA((count,)),
            pltpu.SemaphoreType.DMA,
        ],
        cost_estimate=pl.CostEstimate(flops=400_000_000, bytes_accessed=11_000_000, transcendentals=0),
        name="encode_rest",
    )(tg, og, tu, ou, before)


def decode_kernel(
    first, rest, out_g, out_u, scale_g, scale_u, pick, sums, ready, sems, scales, scale_sems, *pairs
):
    spreads, values, totals = pairs[0:2], pairs[2:4], pairs[4:6]
    parts = first.shape[0]
    width = first.shape[1] - 8
    rows = width * PAIR
    tiles = width // 8
    steps = (rest.shape[1] - 8 + width) // rows
    total = parts * LANES // 2
    half = LANES // 2
    lane = lax.broadcasted_iota(jnp.int32, (8, LANES), 1)
    left = lane < half
    sums[...] = jnp.zeros_like(sums)

    source = lax.broadcasted_iota(jnp.int32, pick.shape, 0)
    goal = lax.broadcasted_iota(jnp.int32, pick.shape, 1)
    tile, at = goal // LANES, goal % LANES
    wanted = 32 * (tile % tiles) + 2 * (tile // tiles) + at // half
    pick[...] = (source == wanted).astype(jnp.bfloat16)

    def copies(step):
        where = pl.ds(pl.multiple_of(step * rows, rows), rows)
        return [
            pltpu.make_async_copy(ready.at[step, m], out.at[where, :], sems.at[step, m])
            for m, out in enumerate((out_g, out_u))
        ]

    def spread_norms(step, side):
        norm = rest[:, steps * rows - width :, :].reshape(parts * 8, LANES).astype(jnp.float32)
        norm = pltpu.roll(norm, lax.rem(LANES - 2 * PAIR * step, LANES), 1)
        spreads[side][...] = jnp.dot(
            norm.astype(jnp.bfloat16), pick[...], preferred_element_type=jnp.float32
        )

    def read(step, side, codes_of):
        acc = [jnp.zeros((8, LANES), jnp.float32) for _ in range(PAIR * tiles)]
        for src in range(parts):
            whole = codes_of(src).astype(jnp.float32)
            for k in range(PAIR * tiles):
                c = whole[8 * k : 8 * k + 8]
                scale = spreads[side][src * 8 : src * 8 + 8, k * LANES : (k + 1) * LANES]
                size = jnp.log2(jnp.maximum(jnp.abs(c), SMALLEST))
                value = (c * jnp.exp2(size * (1.0 / POWER - 1.0))) * scale
                acc[k] = acc[k] + jnp.abs(value)
                values[side][src, 8 * k : 8 * k + 8, :] = value
        for k in range(PAIR * tiles):
            totals[side][8 * k : 8 * k + 8, :] = acc[k]

    def write(step, side):
        factor = []
        for k in range(PAIR * tiles):
            at = slice(8 * k, 8 * k + 8)
            acc = totals[side][at, :]
            sg = jnp.sum(jnp.where(left, acc, 0.0), axis=1, keepdims=True) * (1.0 / total)
            su = jnp.sum(jnp.where(left, 0.0, acc), axis=1, keepdims=True) * (1.0 / total)
            sums[at, :] += jnp.where(
                lane == 2 * step, sg, jnp.where(lane == 2 * step + 1, su, 0.0)
            )
            factor.append(1.0 / jnp.where(left, sg, su))
        for t in range(parts // 2):
            for k in range(PAIR * tiles):
                at = slice(8 * k, 8 * k + 8)
                even = values[side][2 * t, at, :] * factor[k]
                odd = values[side][2 * t + 1, at, :] * factor[k]
                g = jnp.where(left, even, pltpu.roll(odd, half, 1))
                u = jnp.where(left, pltpu.roll(even, half, 1), odd)
                for m, whole in enumerate((g, u)):
                    ready[step, m, at, t * LANES : (t + 1) * LANES] = whole.astype(jnp.bfloat16)
        for copy in copies(step):
            copy.start()

    def from_rest(step, side):
        start = pl.multiple_of(step * rows - width, 8)
        read(step, side, lambda src: rest[src, pl.ds(start, rows), :])

    spread_norms(jnp.int32(0), 0)
    spread_norms(jnp.int32(1), 1)
    read(
        jnp.int32(0),
        0,
        lambda src: jnp.concatenate([first[src, :width, :], rest[src, :width, :]], axis=0),
    )

    @pl.loop(0, steps // 2 - 1)
    def _(i):
        for side in (1, 0):
            step = 2 * i + 2 - side
            write(step - 1, 1 - side)
            spread_norms(step + 1, 1 - side)
            from_rest(step, side)

    last = steps - 1
    write(last - 1, 0)
    from_rest(jnp.int32(last), 1)
    write(last, 1)
    turned = jnp.concatenate(
        [sums[...], jnp.zeros((LANES - rows, LANES), jnp.float32)], axis=0
    ).T
    turned = turned[: 2 * steps].reshape(steps, 2, LANES)
    scale_copies = []
    for m, out in enumerate((scale_g, scale_u)):
        for p in range(PAIR):
            scales[m, pl.ds(p, steps, stride=PAIR), :] = turned[:, m, p * width : (p + 1) * width]
        scale_copies.append(pltpu.make_async_copy(scales.at[m], out, scale_sems.at[m]))
        scale_copies[m].start()
    for copy in scale_copies:
        copy.wait()

    @pl.loop(0, steps)
    def _(step):
        for copy in copies(step):
            copy.wait()


def decode(experts, first, rest):
    parts, rows, lanes = first.shape
    width = rows - 8
    rows = width * PAIR
    total = parts * lanes // 2
    steps = experts // PAIR
    ready = jax.ShapeDtypeStruct((experts * width, total), jnp.bfloat16)
    scale = jax.ShapeDtypeStruct((experts, width), jnp.float32)
    vmem, anywhere = pl.BlockSpec(memory_space=pltpu.VMEM), pl.BlockSpec(memory_space=pl.ANY)
    ready_g, ready_u, scale_g, scale_u = pl.pallas_call(
        decode_kernel,
        in_specs=[vmem, vmem],
        out_specs=[anywhere] * 4,
        out_shape=[ready, ready, scale, scale],
        scratch_shapes=[
            pltpu.VMEM((lanes, rows // 8 * lanes), jnp.bfloat16),
            pltpu.VMEM((rows, lanes), jnp.float32),
            pltpu.VMEM((steps, 2, rows, total), jnp.bfloat16),
            pltpu.SemaphoreType.DMA((steps, 2)),
            pltpu.VMEM((2, experts, width), jnp.float32),
            pltpu.SemaphoreType.DMA((2,)),
            *[pltpu.VMEM((parts * 8, rows // 8 * lanes), jnp.float32)] * 2,
            *[pltpu.VMEM((parts, rows, lanes), jnp.float32)] * 2,
            *[pltpu.VMEM((rows, lanes), jnp.float32)] * 2,
        ],
        compiler_params=pltpu.CompilerParams(vmem_limit_bytes=20 * MIB),
        cost_estimate=pl.CostEstimate(
            flops=400_000_000, bytes_accessed=6_400_000, transcendentals=3_200_000
        ),
        name="decode",
    )(first, rest)
    back = lambda a: jnp.swapaxes(a.reshape(experts, width, total), 1, 2)
    return back(ready_g), back(ready_u), scale_g, scale_u


def gathered(block, axis):
    n, held = lax.axis_size(axis), block[None]
    bit = n // 2
    while bit:
        other = lax.ppermute(held, axis, [(i, i ^ bit) for i in range(n)])
        high = (lax.axis_index(axis) & bit) != 0
        low, top = jnp.where(high, other, held), jnp.where(high, held, other)
        held = jnp.stack([low, top], axis=1).reshape(-1, *block.shape)
        bit //= 2
    return held


def per_device(train_gate, other_gate, train_up, other_up, router_weight, router_gain):
    experts = train_gate.shape[0]
    parts = lax.axis_size("fsdp")
    latest = (train_gate, other_gate, train_up, other_up)
    sent = lambda a: lax.all_to_all(a, "fsdp", split_axis=0, concat_axis=0, tiled=True)

    codes, norms = encode_first(parts, *latest, router_weight.T, router_gain[None])
    first = sent(codes)
    rest = sent(encode_rest(parts, *latest, norms))

    router = gathered(first[:, -8:, :], "ep")
    groups, half = router.shape[0], LANES // 2
    router = router.reshape(groups, parts, 8, 2, half).transpose(1, 4, 0, 3, 2)
    serve_router = router.reshape(parts * half, groups * 16)

    return (*decode(experts, first, rest), serve_router)


def solution(mesh):
    in_specs = (
        P("ep", "fsdp", None),
        P("ep", "fsdp", None),
        P("ep", "fsdp", None),
        P("ep", "fsdp", None),
        P("fsdp", "ep"),
        P("fsdp"),
    )
    out_specs = (
        P("ep", None, "fsdp"),
        P("ep", None, "fsdp"),
        P("ep", "fsdp"),
        P("ep", "fsdp"),
        P(),
    )
    return jax.shard_map(
        per_device, mesh=mesh, in_specs=in_specs, out_specs=out_specs, check_vma=False
    )
```

```python
import functools

import jax
import jax.numpy as jnp
from jax import lax
from jax.experimental import pallas as pl
from jax.experimental.pallas import tpu as pltpu
from jax.sharding import PartitionSpec as P

POWER = 15
SPREAD = 5.0
LEAST = 1e-30
SMALLEST = 2.0**-126
PAIR = 2
LANES = 128
MIB = 2**20


def coded(latest):
    mean = jnp.sum(jnp.abs(latest), axis=0, keepdims=True) * (1.0 / (latest.shape[0] * SPREAD))
    norm = jnp.maximum(mean, LEAST).astype(jnp.bfloat16).astype(jnp.float32)
    v = latest * (1.0 / norm)
    v2 = v * v
    v4 = v2 * v2
    v8 = v4 * v4
    return (v8 * v4) * (v2 * v), norm


def backwards(blocks):
    return jnp.concatenate([blocks[k : k + 1] for k in reversed(range(len(blocks)))], axis=0)


def coded_expert(parts, tg, og, tu, ou):
    cg, ng = coded(tg[...] + og[...].astype(jnp.float32))
    cu, nu = coded(tu[...] + ou[...].astype(jnp.float32))
    codes = jnp.concatenate([cg, cu], axis=0).T.reshape(parts, -1, LANES)
    return backwards(codes), ng, nu


def first_kernel(parts, tg, og, tu, ou, weight, gain, out, norms):
    width = tg.shape[2] // parts
    norms[...] = jnp.zeros_like(norms)
    part = weight[...] * gain[...]
    part = jnp.concatenate([part[:8], part[8:]], axis=1).astype(jnp.bfloat16)
    out[:, width:, :] = jnp.broadcast_to(part[None], (parts, 8, LANES))
    codes, norms[0:1, :], norms[1:2, :] = coded_expert(
        parts, *(a.at[0] for a in (tg, og, tu, ou))
    )
    for k in range(0, width, 8):
        out[:, k : k + 8, :] = codes[:, k : k + 8].astype(jnp.bfloat16)


def encode_first(parts, tg, og, tu, ou, weight, gain):
    _, mine, columns = tg.shape
    width = columns // parts
    block = lambda: pl.BlockSpec((1, mine, columns), lambda s: (0, 0, 0))
    whole = lambda a: pl.BlockSpec(a.shape, lambda s: (0,) * len(a.shape))
    out = jax.ShapeDtypeStruct((parts, width + 8, LANES), jnp.bfloat16)
    norms = jax.ShapeDtypeStruct((8, columns), jnp.float32)
    return pl.pallas_call(
        functools.partial(first_kernel, parts),
        grid=(1,),
        in_specs=[block() for _ in range(4)] + [whole(weight), whole(gain)],
        out_specs=[whole(out), whole(norms)],
        out_shape=[out, norms],
        cost_estimate=pl.CostEstimate(flops=25_000_000, bytes_accessed=900_000, transcendentals=0),
        name="encode_first",
    )(tg, og, tu, ou, weight, gain)


def rest_kernel(parts, tg, og, tu, ou, before, out, ins, codes, norms, norm_rows, in_sems, sems, norm_sem):
    count = codes.shape[0]
    width = codes.shape[2]

    def reads(e):
        return [
            pltpu.make_async_copy(a.at[e + 1], held.at[e], in_sems.at[e, m])
            for m, (a, held) in enumerate(zip((tg, og, tu, ou), ins))
        ]

    def copy(e):
        return pltpu.make_async_copy(
            codes.at[e], out.at[:, pl.ds(pl.multiple_of(e * width, 8), width), :], sems.at[e]
        )

    @pl.loop(0, count)
    def _(e):
        for read in reads(e):
            read.start()

    norms[...] = jnp.zeros_like(norms)
    norms[0:8, :] = before[...]

    @pl.loop(0, count)
    def _(e):
        for read in reads(e):
            read.wait()
        turned, ng, nu = coded_expert(parts, *(held.at[e] for held in ins))
        for k in range(0, width, 8):
            codes[e, :, k : k + 8, :] = turned[:, k : k + 8].astype(jnp.bfloat16)
        norms[pl.ds(2 * e + 2, 1), :] = ng
        norms[pl.ds(2 * e + 3, 1), :] = nu
        copy(e).start()

    turned = norms[...].T.reshape(parts, width // 8, 8, LANES)
    packed = turned[:, 0]
    for k in range(1, width // 8):
        packed = packed + pltpu.roll(turned[:, k], 32 * k, 2)
    norm_rows[...] = backwards(packed).astype(jnp.bfloat16)
    last = pltpu.make_async_copy(norm_rows, out.at[:, pl.ds(count * width, 8), :], norm_sem)
    last.start()

    @pl.loop(0, count)
    def _(e):
        copy(e).wait()

    last.wait()


def encode_rest(parts, tg, og, tu, ou, before):
    experts, mine, columns = tg.shape
    width = columns // parts
    count = experts - 1
    vmem, anywhere = pl.BlockSpec(memory_space=pltpu.VMEM), pl.BlockSpec(memory_space=pl.ANY)

    def kernel(tg, og, tu, ou, before, out, a, b, c, d, *scratch):
        rest_kernel(parts, tg, og, tu, ou, before, out, (a, b, c, d), *scratch)

    return pl.pallas_call(
        kernel,
        in_specs=[anywhere] * 4 + [vmem],
        out_specs=anywhere,
        out_shape=jax.ShapeDtypeStruct((parts, count * width + 8, LANES), jnp.bfloat16),
        scratch_shapes=[
            *[pltpu.VMEM((count, mine, columns), a.dtype) for a in (tg, og, tu, ou)],
            pltpu.VMEM((count, parts, width, LANES), jnp.bfloat16),
            pltpu.VMEM((LANES, columns), jnp.float32),
            pltpu.VMEM((parts, 8, LANES), jnp.bfloat16),
            pltpu.SemaphoreType.DMA((count, 4)),
            pltpu.SemaphoreType.DMA((count,)),
            pltpu.SemaphoreType.DMA,
        ],
        cost_estimate=pl.CostEstimate(flops=400_000_000, bytes_accessed=11_000_000, transcendentals=0),
        name="encode_rest",
    )(tg, og, tu, ou, before)


def decode_kernel(
    first, rest, out_g, out_u, scale_g, scale_u, pick, sums, ready, sems, scales, scale_sems, *pairs
):
    spreads, values, totals = pairs[0:2], pairs[2:4], pairs[4:6]
    parts = first.shape[0]
    width = first.shape[1] - 8
    rows = width * PAIR
    tiles = width // 8
    steps = (rest.shape[1] - 8 + width) // rows
    total = parts * LANES // 2
    half = LANES // 2
    lane = lax.broadcasted_iota(jnp.int32, (8, LANES), 1)
    left = lane < half
    sums[...] = jnp.zeros_like(sums)

    source = lax.broadcasted_iota(jnp.int32, pick.shape, 0)
    goal = lax.broadcasted_iota(jnp.int32, pick.shape, 1)
    tile, at = goal // LANES, goal % LANES
    wanted = 32 * (tile % tiles) + 2 * (tile // tiles) + at // half
    pick[...] = (source == wanted).astype(jnp.bfloat16)

    def copies(step):
        where = pl.ds(pl.multiple_of(step * rows, rows), rows)
        return [
            pltpu.make_async_copy(ready.at[step, m], out.at[where, :], sems.at[step, m])
            for m, out in enumerate((out_g, out_u))
        ]

    def spread_norms(step, side):
        norm = rest[:, steps * rows - width :, :].reshape(parts * 8, LANES).astype(jnp.float32)
        norm = pltpu.roll(norm, lax.rem(LANES - 2 * PAIR * step, LANES), 1)
        spreads[side][...] = jnp.dot(
            norm.astype(jnp.bfloat16), pick[...], preferred_element_type=jnp.float32
        )

    def read(step, side, codes_of):
        acc = [jnp.zeros((8, LANES), jnp.float32) for _ in range(PAIR * tiles)]
        for src in range(parts):
            block = parts - 1 - src
            whole = codes_of(block).astype(jnp.float32)
            for k in range(PAIR * tiles):
                c = whole[8 * k : 8 * k + 8]
                scale = spreads[side][block * 8 : block * 8 + 8, k * LANES : (k + 1) * LANES]
                size = jnp.log2(jnp.maximum(jnp.abs(c), SMALLEST))
                value = (c * jnp.exp2(size * (1.0 / POWER - 1.0))) * scale
                acc[k] = acc[k] + jnp.abs(value)
                values[side][src, 8 * k : 8 * k + 8, :] = value
        for k in range(PAIR * tiles):
            totals[side][8 * k : 8 * k + 8, :] = acc[k]

    def write(step, side):
        factor = []
        for k in range(PAIR * tiles):
            at = slice(8 * k, 8 * k + 8)
            acc = totals[side][at, :]
            sg = jnp.sum(jnp.where(left, acc, 0.0), axis=1, keepdims=True) * (1.0 / total)
            su = jnp.sum(jnp.where(left, 0.0, acc), axis=1, keepdims=True) * (1.0 / total)
            sums[at, :] += jnp.where(
                lane == 2 * step, sg, jnp.where(lane == 2 * step + 1, su, 0.0)
            )
            factor.append(1.0 / jnp.where(left, sg, su))
        for t in range(parts // 2):
            for k in range(PAIR * tiles):
                at = slice(8 * k, 8 * k + 8)
                even = values[side][2 * t, at, :] * factor[k]
                odd = values[side][2 * t + 1, at, :] * factor[k]
                g = jnp.where(left, even, pltpu.roll(odd, half, 1))
                u = jnp.where(left, pltpu.roll(even, half, 1), odd)
                for m, whole in enumerate((g, u)):
                    ready[step, m, at, t * LANES : (t + 1) * LANES] = whole.astype(jnp.bfloat16)
        for copy in copies(step):
            copy.start()

    def from_rest(step, side):
        start = pl.multiple_of(step * rows - width, 8)
        read(step, side, lambda block: rest[block, pl.ds(start, rows), :])

    spread_norms(jnp.int32(0), 0)
    spread_norms(jnp.int32(1), 1)
    read(
        jnp.int32(0),
        0,
        lambda block: jnp.concatenate([first[block, :width, :], rest[block, :width, :]], axis=0),
    )

    @pl.loop(0, steps // 2 - 1)
    def _(i):
        for side in (1, 0):
            step = 2 * i + 2 - side
            write(step - 1, 1 - side)
            spread_norms(step + 1, 1 - side)
            from_rest(step, side)

    last = steps - 1
    write(last - 1, 0)
    from_rest(jnp.int32(last), 1)
    write(last, 1)
    turned = jnp.concatenate(
        [sums[...], jnp.zeros((LANES - rows, LANES), jnp.float32)], axis=0
    ).T
    turned = turned[: 2 * steps].reshape(steps, 2, LANES)
    scale_copies = []
    for m, out in enumerate((scale_g, scale_u)):
        for p in range(PAIR):
            scales[m, pl.ds(p, steps, stride=PAIR), :] = turned[:, m, p * width : (p + 1) * width]
        scale_copies.append(pltpu.make_async_copy(scales.at[m], out, scale_sems.at[m]))
        scale_copies[m].start()
    for copy in scale_copies:
        copy.wait()

    @pl.loop(0, steps)
    def _(step):
        for copy in copies(step):
            copy.wait()


def decode(experts, first, rest):
    parts, rows, lanes = first.shape
    width = rows - 8
    rows = width * PAIR
    total = parts * lanes // 2
    steps = experts // PAIR
    ready = jax.ShapeDtypeStruct((experts * width, total), jnp.bfloat16)
    scale = jax.ShapeDtypeStruct((experts, width), jnp.float32)
    vmem, anywhere = pl.BlockSpec(memory_space=pltpu.VMEM), pl.BlockSpec(memory_space=pl.ANY)
    ready_g, ready_u, scale_g, scale_u = pl.pallas_call(
        decode_kernel,
        in_specs=[vmem, vmem],
        out_specs=[anywhere] * 4,
        out_shape=[ready, ready, scale, scale],
        scratch_shapes=[
            pltpu.VMEM((lanes, rows // 8 * lanes), jnp.bfloat16),
            pltpu.VMEM((rows, lanes), jnp.float32),
            pltpu.VMEM((steps, 2, rows, total), jnp.bfloat16),
            pltpu.SemaphoreType.DMA((steps, 2)),
            pltpu.VMEM((2, experts, width), jnp.float32),
            pltpu.SemaphoreType.DMA((2,)),
            *[pltpu.VMEM((parts * 8, rows // 8 * lanes), jnp.float32)] * 2,
            *[pltpu.VMEM((parts, rows, lanes), jnp.float32)] * 2,
            *[pltpu.VMEM((rows, lanes), jnp.float32)] * 2,
        ],
        compiler_params=pltpu.CompilerParams(vmem_limit_bytes=20 * MIB),
        cost_estimate=pl.CostEstimate(
            flops=400_000_000, bytes_accessed=6_400_000, transcendentals=3_200_000
        ),
        name="decode",
    )(first, rest)
    back = lambda a: jnp.swapaxes(a.reshape(experts, width, total), 1, 2)
    return back(ready_g), back(ready_u), scale_g, scale_u


def gathered(block, axis):
    n, held = lax.axis_size(axis), block[None]
    bit = n // 2
    while bit:
        other = lax.ppermute(held, axis, [(i, i ^ bit) for i in range(n)])
        high = (lax.axis_index(axis) & bit) != 0
        low, top = jnp.where(high, other, held), jnp.where(high, held, other)
        held = jnp.stack([low, top], axis=1).reshape(-1, *block.shape)
        bit //= 2
    return held


def per_device(train_gate, other_gate, train_up, other_up, router_weight, router_gain):
    experts = train_gate.shape[0]
    parts = lax.axis_size("fsdp")
    latest = (train_gate, other_gate, train_up, other_up)
    order = [list(range(parts))[::-1]]
    sent = lambda a: lax.all_to_all(
        a, "fsdp", split_axis=0, concat_axis=0, axis_index_groups=order, tiled=True
    )

    codes, norms = encode_first(parts, *latest, router_weight.T, router_gain[None])
    first = sent(codes)
    rest = sent(encode_rest(parts, *latest, norms))

    router = gathered(first[::-1, -8:, :], "ep")
    groups, half = router.shape[0], LANES // 2
    router = router.reshape(groups, parts, 8, 2, half).transpose(1, 4, 0, 3, 2)
    serve_router = router.reshape(parts * half, groups * 16)

    return (*decode(experts, first, rest), serve_router)


def solution(mesh):
    in_specs = (
        P("ep", "fsdp", None),
        P("ep", "fsdp", None),
        P("ep", "fsdp", None),
        P("ep", "fsdp", None),
        P("fsdp", "ep"),
        P("fsdp"),
    )
    out_specs = (
        P("ep", None, "fsdp"),
        P("ep", None, "fsdp"),
        P("ep", "fsdp"),
        P("ep", "fsdp"),
        P(),
    )
    return jax.shard_map(
        per_device, mesh=mesh, in_specs=in_specs, out_specs=out_specs, check_vma=False
    )
```

```python
import functools

import jax
import jax.numpy as jnp
from jax import lax
from jax.experimental import pallas as pl
from jax.experimental.pallas import tpu as pltpu
from jax.sharding import PartitionSpec as P

POWER = 15
SPREAD = 5.0
LEAST = 1e-30
SMALLEST = 2.0**-126
PAIR = 2
LANES = 128
MIB = 2**20


def coded(latest):
    mean = jnp.sum(jnp.abs(latest), axis=0, keepdims=True) * (1.0 / (latest.shape[0] * SPREAD))
    norm = jnp.maximum(mean, LEAST).astype(jnp.bfloat16).astype(jnp.float32)
    v = latest * (1.0 / norm)
    v2 = v * v
    v4 = v2 * v2
    v8 = v4 * v4
    return (v8 * v4) * (v2 * v), norm


def swapped(blocks, at=4):
    return [*blocks[at : 2 * at], *blocks[:at], *blocks[2 * at :]]


def backwards(blocks):
    return jnp.concatenate([blocks[k : k + 1] for k in reversed(range(len(blocks)))], axis=0)


def coded_expert(parts, tg, og, tu, ou):
    cg, ng = coded(tg[...] + og[...].astype(jnp.float32))
    cu, nu = coded(tu[...] + ou[...].astype(jnp.float32))
    codes = jnp.concatenate([cg, cu], axis=0).T.reshape(parts, -1, LANES)
    return backwards(codes), ng, nu


def first_kernel(parts, tg, og, tu, ou, weight, gain, out, norms):
    width = tg.shape[2] // parts
    norms[...] = jnp.zeros_like(norms)
    part = weight[...] * gain[...]
    part = jnp.concatenate([part[:8], part[8:]], axis=1).astype(jnp.bfloat16)
    out[:, width:, :] = jnp.broadcast_to(part[None], (parts, 8, LANES))
    codes, norms[0:1, :], norms[1:2, :] = coded_expert(
        parts, *(a.at[0] for a in (tg, og, tu, ou))
    )
    codes = jnp.concatenate([codes[b : b + 1] for b in swapped(range(parts))], axis=0)
    for k in range(0, width, 8):
        out[:, k : k + 8, :] = codes[:, k : k + 8].astype(jnp.bfloat16)


def encode_first(parts, tg, og, tu, ou, weight, gain):
    _, mine, columns = tg.shape
    width = columns // parts
    block = lambda: pl.BlockSpec((1, mine, columns), lambda s: (0, 0, 0))
    whole = lambda a: pl.BlockSpec(a.shape, lambda s: (0,) * len(a.shape))
    out = jax.ShapeDtypeStruct((parts, width + 8, LANES), jnp.bfloat16)
    norms = jax.ShapeDtypeStruct((8, columns), jnp.float32)
    return pl.pallas_call(
        functools.partial(first_kernel, parts),
        grid=(1,),
        in_specs=[block() for _ in range(4)] + [whole(weight), whole(gain)],
        out_specs=[whole(out), whole(norms)],
        out_shape=[out, norms],
        cost_estimate=pl.CostEstimate(flops=25_000_000, bytes_accessed=900_000, transcendentals=0),
        name="encode_first",
    )(tg, og, tu, ou, weight, gain)


def rest_kernel(parts, tg, og, tu, ou, before, out, ins, codes, norms, norm_rows, in_sems, sems, norm_sem):
    count = codes.shape[0]
    width = codes.shape[2]

    def reads(e):
        return [
            pltpu.make_async_copy(a.at[e + 1], held.at[e], in_sems.at[e, m])
            for m, (a, held) in enumerate(zip((tg, og, tu, ou), ins))
        ]

    def copy(e):
        return pltpu.make_async_copy(
            codes.at[e], out.at[:, pl.ds(pl.multiple_of(e * width, 8), width), :], sems.at[e]
        )

    @pl.loop(0, count)
    def _(e):
        for read in reads(e):
            read.start()

    norms[...] = jnp.zeros_like(norms)
    norms[0:8, :] = before[...]

    @pl.loop(0, count)
    def _(e):
        for read in reads(e):
            read.wait()
        turned, ng, nu = coded_expert(parts, *(held.at[e] for held in ins))
        for k in range(0, width, 8):
            codes[e, :, k : k + 8, :] = turned[:, k : k + 8].astype(jnp.bfloat16)
        norms[pl.ds(2 * e + 2, 1), :] = ng
        norms[pl.ds(2 * e + 3, 1), :] = nu
        copy(e).start()

    turned = norms[...].T.reshape(parts, width // 8, 8, LANES)
    packed = turned[:, 0]
    for k in range(1, width // 8):
        packed = packed + pltpu.roll(turned[:, k], 32 * k, 2)
    norm_rows[...] = backwards(packed).astype(jnp.bfloat16)
    last = pltpu.make_async_copy(norm_rows, out.at[:, pl.ds(count * width, 8), :], norm_sem)
    last.start()

    @pl.loop(0, count)
    def _(e):
        copy(e).wait()

    last.wait()


def encode_rest(parts, tg, og, tu, ou, before):
    experts, mine, columns = tg.shape
    width = columns // parts
    count = experts - 1
    vmem, anywhere = pl.BlockSpec(memory_space=pltpu.VMEM), pl.BlockSpec(memory_space=pl.ANY)

    def kernel(tg, og, tu, ou, before, out, a, b, c, d, *scratch):
        rest_kernel(parts, tg, og, tu, ou, before, out, (a, b, c, d), *scratch)

    return pl.pallas_call(
        kernel,
        in_specs=[anywhere] * 4 + [vmem],
        out_specs=anywhere,
        out_shape=jax.ShapeDtypeStruct((parts, count * width + 8, LANES), jnp.bfloat16),
        scratch_shapes=[
            *[pltpu.VMEM((count, mine, columns), a.dtype) for a in (tg, og, tu, ou)],
            pltpu.VMEM((count, parts, width, LANES), jnp.bfloat16),
            pltpu.VMEM((LANES, columns), jnp.float32),
            pltpu.VMEM((parts, 8, LANES), jnp.bfloat16),
            pltpu.SemaphoreType.DMA((count, 4)),
            pltpu.SemaphoreType.DMA((count,)),
            pltpu.SemaphoreType.DMA,
        ],
        cost_estimate=pl.CostEstimate(flops=400_000_000, bytes_accessed=11_000_000, transcendentals=0),
        name="encode_rest",
    )(tg, og, tu, ou, before)


def decode_kernel(
    first, rest, out_g, out_u, scale_g, scale_u, pick, sums, ready, sems, scales, scale_sems, *pairs
):
    spreads, values, totals = pairs[0:2], pairs[2:4], pairs[4:6]
    parts = first.shape[0]
    width = first.shape[1] - 8
    rows = width * PAIR
    tiles = width // 8
    steps = (rest.shape[1] - 8 + width) // rows
    total = parts * LANES // 2
    half = LANES // 2
    lane = lax.broadcasted_iota(jnp.int32, (8, LANES), 1)
    left = lane < half
    sums[...] = jnp.zeros_like(sums)

    source = lax.broadcasted_iota(jnp.int32, pick.shape, 0)
    goal = lax.broadcasted_iota(jnp.int32, pick.shape, 1)
    tile, at = goal // LANES, goal % LANES
    wanted = 32 * (tile % tiles) + 2 * (tile // tiles) + at // half
    pick[...] = (source == wanted).astype(jnp.bfloat16)

    def copies(step):
        where = pl.ds(pl.multiple_of(step * rows, rows), rows)
        return [
            pltpu.make_async_copy(ready.at[step, m], out.at[where, :], sems.at[step, m])
            for m, out in enumerate((out_g, out_u))
        ]

    def spread_norms(step, side):
        norm = rest[:, steps * rows - width :, :].reshape(parts * 8, LANES).astype(jnp.float32)
        norm = pltpu.roll(norm, lax.rem(LANES - 2 * PAIR * step, LANES), 1)
        spreads[side][...] = jnp.dot(
            norm.astype(jnp.bfloat16), pick[...], preferred_element_type=jnp.float32
        )

    def read(step, side, codes_of):
        acc = [jnp.zeros((8, LANES), jnp.float32) for _ in range(PAIR * tiles)]
        for src in range(parts):
            block = parts - 1 - src
            whole = codes_of(block).astype(jnp.float32)
            for k in range(PAIR * tiles):
                c = whole[8 * k : 8 * k + 8]
                scale = spreads[side][block * 8 : block * 8 + 8, k * LANES : (k + 1) * LANES]
                size = jnp.log2(jnp.maximum(jnp.abs(c), SMALLEST))
                value = (c * jnp.exp2(size * (1.0 / POWER - 1.0))) * scale
                acc[k] = acc[k] + jnp.abs(value)
                values[side][src, 8 * k : 8 * k + 8, :] = value
        for k in range(PAIR * tiles):
            totals[side][8 * k : 8 * k + 8, :] = acc[k]

    def write(step, side):
        factor = []
        for k in range(PAIR * tiles):
            at = slice(8 * k, 8 * k + 8)
            acc = totals[side][at, :]
            sg = jnp.sum(jnp.where(left, acc, 0.0), axis=1, keepdims=True) * (1.0 / total)
            su = jnp.sum(jnp.where(left, 0.0, acc), axis=1, keepdims=True) * (1.0 / total)
            sums[at, :] += jnp.where(
                lane == 2 * step, sg, jnp.where(lane == 2 * step + 1, su, 0.0)
            )
            factor.append(1.0 / jnp.where(left, sg, su))
        for t in range(parts // 2):
            for k in range(PAIR * tiles):
                at = slice(8 * k, 8 * k + 8)
                even = values[side][2 * t, at, :] * factor[k]
                odd = values[side][2 * t + 1, at, :] * factor[k]
                g = jnp.where(left, even, pltpu.roll(odd, half, 1))
                u = jnp.where(left, pltpu.roll(even, half, 1), odd)
                for m, whole in enumerate((g, u)):
                    ready[step, m, at, t * LANES : (t + 1) * LANES] = whole.astype(jnp.bfloat16)
        for copy in copies(step):
            copy.start()

    def from_rest(step, side):
        start = pl.multiple_of(step * rows - width, 8)
        read(step, side, lambda block: rest[block, pl.ds(start, rows), :])

    spread_norms(jnp.int32(0), 0)
    spread_norms(jnp.int32(1), 1)
    read(
        jnp.int32(0),
        0,
        lambda block: jnp.concatenate(
            [first[swapped(range(parts))[block], :width, :], rest[block, :width, :]], axis=0
        ),
    )

    @pl.loop(0, steps // 2 - 1)
    def _(i):
        for side in (1, 0):
            step = 2 * i + 2 - side
            write(step - 1, 1 - side)
            spread_norms(step + 1, 1 - side)
            from_rest(step, side)

    last = steps - 1
    write(last - 1, 0)
    from_rest(jnp.int32(last), 1)
    write(last, 1)
    turned = jnp.concatenate(
        [sums[...], jnp.zeros((LANES - rows, LANES), jnp.float32)], axis=0
    ).T
    turned = turned[: 2 * steps].reshape(steps, 2, LANES)
    scale_copies = []
    for m, out in enumerate((scale_g, scale_u)):
        for p in range(PAIR):
            scales[m, pl.ds(p, steps, stride=PAIR), :] = turned[:, m, p * width : (p + 1) * width]
        scale_copies.append(pltpu.make_async_copy(scales.at[m], out, scale_sems.at[m]))
        scale_copies[m].start()
    for copy in scale_copies:
        copy.wait()

    @pl.loop(0, steps)
    def _(step):
        for copy in copies(step):
            copy.wait()


def decode(experts, first, rest):
    parts, rows, lanes = first.shape
    width = rows - 8
    rows = width * PAIR
    total = parts * lanes // 2
    steps = experts // PAIR
    ready = jax.ShapeDtypeStruct((experts * width, total), jnp.bfloat16)
    scale = jax.ShapeDtypeStruct((experts, width), jnp.float32)
    vmem, anywhere = pl.BlockSpec(memory_space=pltpu.VMEM), pl.BlockSpec(memory_space=pl.ANY)
    ready_g, ready_u, scale_g, scale_u = pl.pallas_call(
        decode_kernel,
        in_specs=[vmem, vmem],
        out_specs=[anywhere] * 4,
        out_shape=[ready, ready, scale, scale],
        scratch_shapes=[
            pltpu.VMEM((lanes, rows // 8 * lanes), jnp.bfloat16),
            pltpu.VMEM((rows, lanes), jnp.float32),
            pltpu.VMEM((steps, 2, rows, total), jnp.bfloat16),
            pltpu.SemaphoreType.DMA((steps, 2)),
            pltpu.VMEM((2, experts, width), jnp.float32),
            pltpu.SemaphoreType.DMA((2,)),
            *[pltpu.VMEM((parts * 8, rows // 8 * lanes), jnp.float32)] * 2,
            *[pltpu.VMEM((parts, rows, lanes), jnp.float32)] * 2,
            *[pltpu.VMEM((rows, lanes), jnp.float32)] * 2,
        ],
        compiler_params=pltpu.CompilerParams(vmem_limit_bytes=20 * MIB),
        cost_estimate=pl.CostEstimate(
            flops=400_000_000, bytes_accessed=6_400_000, transcendentals=3_200_000
        ),
        name="decode",
    )(first, rest)
    back = lambda a: jnp.swapaxes(a.reshape(experts, width, total), 1, 2)
    return back(ready_g), back(ready_u), scale_g, scale_u


def gathered(block, axis):
    n, held = lax.axis_size(axis), block[None]
    bit = n // 2
    while bit:
        other = lax.ppermute(held, axis, [(i, i ^ bit) for i in range(n)])
        high = (lax.axis_index(axis) & bit) != 0
        low, top = jnp.where(high, other, held), jnp.where(high, held, other)
        held = jnp.stack([low, top], axis=1).reshape(-1, *block.shape)
        bit //= 2
    return held


def per_device(train_gate, other_gate, train_up, other_up, router_weight, router_gain):
    experts = train_gate.shape[0]
    parts = lax.axis_size("fsdp")
    latest = (train_gate, other_gate, train_up, other_up)
    order = list(range(parts))[::-1]
    sent = lambda a, order: lax.all_to_all(
        a, "fsdp", split_axis=0, concat_axis=0, axis_index_groups=[order], tiled=True
    )

    codes, norms = encode_first(parts, *latest, router_weight.T, router_gain[None])
    first = sent(codes, swapped(order))
    rest = sent(encode_rest(parts, *latest, norms), order)

    router = first[:, -8:, :]
    router = jnp.concatenate([router[4:8], router[:4], router[8:]], axis=0)
    router = gathered(router[::-1], "ep")
    groups, half = router.shape[0], LANES // 2
    router = router.reshape(groups, parts, 8, 2, half).transpose(1, 4, 0, 3, 2)
    serve_router = router.reshape(parts * half, groups * 16)

    return (*decode(experts, first, rest), serve_router)


def solution(mesh):
    in_specs = (
        P("ep", "fsdp", None),
        P("ep", "fsdp", None),
        P("ep", "fsdp", None),
        P("ep", "fsdp", None),
        P("fsdp", "ep"),
        P("fsdp"),
    )
    out_specs = (
        P("ep", None, "fsdp"),
        P("ep", None, "fsdp"),
        P("ep", "fsdp"),
        P("ep", "fsdp"),
        P(),
    )
    return jax.shard_map(
        per_device, mesh=mesh, in_specs=in_specs, out_specs=out_specs, check_vma=False
    )
```
